32 devices in a mesh: seq: 16 (over z, y, x), head: 2 (over core).
Axes of the slice: x: 2, y: 2, z: 4, core: 2. Of those that a mesh axis runs over, the one named last changes fastest.
Arguments:
- queries: bfloat16 [4096, 4096], P('seq', 'head'), may hold values from -210 to 210
- keys: bfloat16 [4096, 1024], P('seq', 'head'), may hold values from -7 to 7
- values: bfloat16 [4096, 1024], P('seq', 'head'), may hold values from -6 to 6
- vertical: int32 [8, 16], P('head'), may hold values from 0 to 63, as said below
- slash: int32 [8, 2], P('head'), may hold values from 1 to 4, as said below
- out_weight: bfloat16 [4096, 4096], P('head'), may hold values from -1 to 1
Outputs:
- mixed: bfloat16 [4096, 4096], P(('seq', 'head'))
The draws below stay inside these ranges and needn't reach their ends.
Inputs may be any that keep to these rules, and one draw needn't show every extreme that they name: `vertical`: for each key-value head, 16 different key blocks in increasing order; block b lies in slab b // 4; no slab holds more than 2 of one head's blocks, and for every head some slab holds exactly 2. `slash`: for each key-value head, 2 different offsets in increasing order; some head has the offset 256 // 64.
All inputs are finite; a program needn't handle non-finite values.
Results may differ from the reference program's by a relative error of at most 0.01.
Values may be sent and summed in bfloat16 or wider, within the bound.
A program may use at most 128 MiB of HBM per device.

```python
from functools import partial
import jax
import jax.numpy as jnp
from jax import lax

HEADS = 32
KEY_VALUE_HEADS = 8
HEAD_DIM = 128
DMODEL = 4096
S_DEV = 256
BLK = 64
NS = 2
CAP = 2
NV = 16
SEQ = 4096
N_SEQ = 16


def paired(key):
    key_seed, query_seed = jax.random.split(jax.random.fold_in(key, 7), 2)
    keys_f = jnp.clip(jax.random.normal(key_seed, (SEQ, KEY_VALUE_HEADS * HEAD_DIM), jnp.float32), -6.0, 6.0)
    query_f = jnp.clip(1.5 * jax.random.normal(query_seed, (SEQ, HEADS * HEAD_DIM), jnp.float32), -9.0, 9.0)
    return (query_f, keys_f)


def draw_queries(key, part):
    return paired(key)[0].astype(jnp.bfloat16)


def draw_keys(key, part):
    return paired(key)[1].astype(jnp.bfloat16)


def draw_vertical(key, part):
    block_span = S_DEV // BLK
    owners = SEQ // S_DEV
    perm_seed, score_seed, force_seed = jax.random.split(jax.random.fold_in(key, 3), 3)
    within = jax.random.randint(perm_seed, (KEY_VALUE_HEADS, owners, block_span), 0, 1 << 20) * block_span + jnp.arange(block_span, dtype=jnp.int32)
    order = jnp.argsort(within, axis=-1)[:, :, :CAP]
    blocks = (order + jnp.arange(owners, dtype=jnp.int32)[None, :, None] * block_span).reshape(KEY_VALUE_HEADS, owners * CAP)
    owner_of = jnp.repeat(jnp.arange(owners, dtype=jnp.int32), CAP)
    forced_blocks = jax.random.randint(force_seed, (KEY_VALUE_HEADS, 1), 0, owners)
    block_score = jax.random.randint(score_seed, (KEY_VALUE_HEADS, owners * CAP), 0, 4096) + (owners - owner_of)[None, :] * (8192 // owners)
    block_score = block_score + jnp.where(owner_of[None, :] == forced_blocks, 1 << 16, 0)
    block_score = block_score * (owners * CAP) + jnp.arange(owners * CAP, dtype=jnp.int32)[None, :]
    unused, picked = lax.top_k(block_score, NV)
    chosen = jnp.take_along_axis(blocks, picked, axis=1)
    return jnp.sort(chosen, axis=1).astype(jnp.int32)


def draw_slash(key, part):
    block_span = S_DEV // BLK
    score_seed, force_seed = jax.random.split(jax.random.fold_in(key, 5), 2)
    block_score = jax.random.randint(score_seed, (KEY_VALUE_HEADS, block_span), 0, 4096) * block_span + jnp.arange(block_span, dtype=jnp.int32)[None, :]
    forced_blocks = jax.random.randint(force_seed, (), 0, KEY_VALUE_HEADS)
    extra_score = (jnp.arange(KEY_VALUE_HEADS)[:, None] == forced_blocks) & (jnp.arange(block_span)[None, :] == block_span - 1)
    block_score = block_score + jnp.where(extra_score, 1 << 24, 0)
    unused, picked = lax.top_k(block_score, NS)
    return jnp.sort(picked + 1, axis=1).astype(jnp.int32)


def block_scale(key, shape, pieces, least, top_value):
    def one(position, blocks):
        steps = jax.random.uniform(jax.random.fold_in(jax.random.fold_in(key, 6), position), (blocks,), jnp.float32, least / len(pieces), top_value / len(pieces))
        return jnp.repeat(jnp.exp(steps), shape[position] // blocks).reshape((-1,) + (1,) * (len(shape) - position - 1))

    loudness = one(*pieces[0])
    for cut in pieces[1:]:
        loudness = loudness * one(*cut)
    return loudness


def bell_draw(key, shape, scale, bound, pieces=(), held_as=jnp.bfloat16):
    factor_of = block_scale(key, shape, pieces, -0.22, 0.18) if pieces else 1.0
    array = jax.random.normal(key, shape, jnp.float32) * scale * factor_of
    return jnp.minimum(jnp.maximum(array, -bound), bound).astype(held_as)


def setup_inputs(seed: int = 0) -> dict:
    splits = jax.random.split(jax.random.key(seed), 7)
    return {
        "queries": draw_queries(jax.random.fold_in(splits[6], 71), 0),
        "keys": draw_keys(jax.random.fold_in(splits[6], 71), 0),
        "values": bell_draw(splits[2], (SEQ, KEY_VALUE_HEADS * HEAD_DIM), 1.0, 6.0, ((0, 16), (1, 2))),
        "vertical": draw_vertical(jax.random.fold_in(splits[6], 71), 0),
        "slash": draw_slash(jax.random.fold_in(splits[6], 71), 0),
        "out_weight": bell_draw(splits[5], (HEADS * HEAD_DIM, DMODEL), HEADS ** -0.5, 1.0, ((0, 2),)),
    }


NEGATIVE = -1e30


def attended_block_tile(block_index, vert_ids, slash_ids, key_head, value_head, query_head_index, causal):
    offsets = jnp.concatenate([jnp.zeros((1,), jnp.int32), slash_ids.astype(jnp.int32)])
    diagonal = block_index - offsets
    vert_ok = (vert_ids < block_index) & jnp.all(block_index - vert_ids[:, None] != slash_ids[None, :], axis=1)
    diag_ok = diagonal >= 0
    chosen = jnp.concatenate([vert_ids.astype(jnp.int32), jnp.maximum(diagonal, 0).astype(jnp.int32)])
    usable = jnp.concatenate([vert_ok, diag_ok])
    gathered_keys = key_head[chosen].reshape(-1, HEAD_DIM)
    gathered_values = value_head[chosen].reshape(-1, HEAD_DIM)
    same_block = chosen == block_index
    allowed = usable[None, :, None] & (jnp.logical_not(same_block)[None, :, None] | causal[:, None, :])
    allowed = allowed.reshape(BLK, -1)
    query_block_tile = query_head_index[block_index]
    scores = jnp.einsum("qgd,kd->gqk", query_block_tile.astype(jnp.float32), gathered_keys.astype(jnp.float32)) * (HEAD_DIM ** -0.5)
    scores = jnp.where(allowed[None], scores, NEGATIVE)
    top_score = jnp.max(scores, axis=-1, keepdims=True)
    weights = jnp.where(allowed[None], jnp.exp(scores - top_score), 0.0)
    sum_weight = jnp.sum(weights, axis=-1, keepdims=True)
    rounded = lax.optimization_barrier(weights.astype(jnp.bfloat16)).astype(jnp.float32)
    output = jnp.einsum("gqk,kd->gqd", rounded, gathered_values.astype(jnp.float32)) / sum_weight
    return output.transpose(1, 0, 2).astype(jnp.bfloat16)


def attend_slab(slab_start, block_fn, slab_blocks):
    return jax.vmap(block_fn)(slab_start + jnp.arange(slab_blocks, dtype=jnp.int32))


def reference(queries, keys, values, vertical, slash, out_weight):
    per_group = HEADS // KEY_VALUE_HEADS
    block_count = SEQ // BLK
    slab_blocks = S_DEV // BLK
    query_blocks = queries.reshape(block_count, BLK, KEY_VALUE_HEADS, per_group, HEAD_DIM)
    key_blocks = keys.reshape(block_count, BLK, KEY_VALUE_HEADS, HEAD_DIM)
    value_blocks = values.reshape(block_count, BLK, KEY_VALUE_HEADS, HEAD_DIM)
    within = jnp.arange(BLK)
    causal = within[None, :] <= within[:, None]
    results = []
    for head_index in range(KEY_VALUE_HEADS):
        block_fn = partial(attended_block_tile, vert_ids=vertical[head_index], slash_ids=slash[head_index],
                           key_head=key_blocks[:, :, head_index], value_head=value_blocks[:, :, head_index],
                           query_head_index=query_blocks[:, :, head_index], causal=causal)
        mapped = lax.map(partial(attend_slab, block_fn=block_fn, slab_blocks=slab_blocks),
                         jnp.arange(N_SEQ, dtype=jnp.int32) * slab_blocks)
        results.append(mapped.reshape(SEQ, per_group * HEAD_DIM))
    attention = jnp.concatenate(results, axis=1)
    return jnp.dot(attention, out_weight, preferred_element_type=jnp.float32).astype(jnp.bfloat16)
```

```python
import functools
import math

import jax
import jax.numpy as jnp
from jax import lax
from jax.experimental import pallas as pl
from jax.experimental.pallas import tpu as pltpu
from jax.sharding import PartitionSpec as P

HEAD_DIM = 128
BLK = 64
CAP = 2
NEGATIVE = -1e30
MESH = pl.DeviceIdType.MESH
SCALE = HEAD_DIM ** (-0.5) * math.log2(math.e)


def kernel(
    n, inner, per_group, tile, grain, middle,
    q_hbm, k_hbm, v_hbm, vert_ref, slash_ref, w_hbm, out_ref,
    qbuf, kbuf, vbuf, prev, inc, pos, vtpos, acc, top, total, abuf, attn, w_ref, res, give, take,
    local_sem, w_sem, k_send, k_recv, v_send, v_recv, q_send, q_recv,
    p_send, p_recv, c_send, c_recv, r_send, r_recv, x_send, x_recv,
):
    slab_blocks = q_hbm.shape[0]
    rows = slab_blocks * BLK
    width = per_group * HEAD_DIM
    outer = n // inner
    me = lax.axis_index("seq")
    core = lax.axis_index("head")
    o, c = me // inner, me % inner
    other = 1 - core
    plane_blocks = inner * slab_blocks
    first = o * plane_blocks
    chosen = vert_ref.shape[1]
    grains = chosen // grain
    slashes = slash_ref.shape[0]
    half = rows // 2
    base = o * inner
    pair = math.gcd(inner, 2)

    def peer(e):
        return ((c // pair + e // pair) % (inner // pair)) * pair + (c % pair + e % pair) % pair

    def source(e):
        up = (c // pair + inner // pair - e // pair) % (inner // pair)
        return up * pair + (c % pair + pair - e % pair) % pair

    barrier = pltpu.get_barrier_semaphore()

    def greet(seq, head):
        pl.semaphore_signal(barrier, inc=1, device_id=(seq, head), device_id_type=MESH)

    greet(me, other)
    for e in range(1, inner):
        greet(base + peer(e), core)

    @pl.when(o < outer - 1)
    def _():
        greet(me + inner, core)

    @pl.when(o > 0)
    def _():
        greet(me - inner, core)

    def span(index, size):
        return pl.ds(pl.multiple_of(index * size, size), size)

    own_copies = [
        pltpu.make_async_copy(hbm.at[:, :, span(c, size)], ref.at[span(c, slab_blocks)], local_sem.at[i])
        for i, (hbm, ref, size) in enumerate(
            ((k_hbm, kbuf, HEAD_DIM), (v_hbm, vbuf, HEAD_DIM), (q_hbm, qbuf, width)))
    ]
    for copy in own_copies:
        copy.start()

    pl.semaphore_wait(
        barrier, inner + jnp.where(o > 0, 1, 0) + jnp.where(o < outer - 1, 1, 0))

    def remote(src, dst, send_sem, recv_sem, seq):
        return pltpu.make_async_remote_copy(
            src_ref=src, dst_ref=dst, send_sem=send_sem, recv_sem=recv_sem,
            device_id=(seq, core), device_id_type=MESH,
        )

    def handed(hbm, ref, size, send_sem, recv_sem, to, slab):
        return remote(hbm.at[:, :, span(to, size)], ref.at[span(slab, slab_blocks)], send_sem,
                      recv_sem.at[slab], base + to)

    def give_k(e):
        return handed(k_hbm, kbuf, HEAD_DIM, k_send.at[e], k_recv, peer(e), c)

    def give_v(e):
        return handed(v_hbm, vbuf, HEAD_DIM, v_send.at[e], v_recv, peer(e), c)

    def give_q(e):
        return handed(q_hbm, qbuf, width, q_send.at[e], q_recv, peer(e), c)

    others = range(inner - 1, 0, -1)
    for e in others:
        give_k(e).start()
        give_v(e).start()
    for e in others:
        give_q(e).start()
    weight_copy = pltpu.make_async_copy(w_hbm, w_ref, w_sem)
    weight_copy.start()

    above = (me + inner) % n

    def chain_copy(g):
        there = pl.ds(pl.multiple_of(g * grain, grain), grain)
        return remote(pos.at[there], inc.at[there], c_send.at[g], c_recv.at[g], above)

    def prev_copy(part):
        ref = (kbuf, vbuf)[part]
        return remote(ref.at[span(inner - 1, slab_blocks)], prev.at[part], p_send.at[part],
                      p_recv.at[part], above)

    def arriving(g):
        return g * grain < CAP * inner * o

    def leaving(g):
        return (o < outer - 1) & (g * grain < CAP * inner * (o + 1))

    def chain(g):
        @pl.when(arriving(g))
        def _():
            chain_copy(g).wait_recv()

        @pl.when(jnp.logical_not(arriving(g)))
        def _():
            there = pl.ds(pl.multiple_of(g * grain, grain), grain)
            inc[there] = jnp.zeros((grain, 2 * BLK, HEAD_DIM), inc.dtype)

        picked = []
        for i in range(grain):
            p = g * grain + i
            at = vert_ref[c, p] - first
            mine = (at >= 0) & (at < plane_blocks)
            here = jnp.clip(at, 0, plane_blocks - 1)
            pos[p, :BLK] = jnp.where(mine, kbuf[here], inc[p, :BLK])
            v = jnp.where(mine, vbuf[here], inc[p, BLK:])
            pos[p, BLK:] = v
            picked.append(v)

        @pl.when(leaving(g))
        def _():
            chain_copy(g).start()

        vtpos[g] = jnp.concatenate(picked, axis=0).T

    def start_prev():
        for part in range(2):
            prev_copy(part).start()

    def queries(a):
        return jnp.concatenate(
            [qbuf[a, :, g * HEAD_DIM:(g + 1) * HEAD_DIM] for g in range(per_group)], axis=0)

    def on_slash(gap):
        hit = gap == slash_ref[0, c]
        for i in range(1, slashes):
            hit = hit | (gap == slash_ref[i, c])
        return hit

    def update(a, k, vt, negs, old, triangle=False):
        s = lax.dot_general(k, queries(a), (((1,), (1,)), ((), ())),
                            preferred_element_type=jnp.float32)
        blocks = [s[i * BLK:(i + 1) * BLK] for i in range(len(negs))]
        if triangle:
            keys_at = lax.broadcasted_iota(jnp.int32, blocks[0].shape, 0)
            query_at = lax.broadcasted_iota(jnp.int32, blocks[0].shape, 1) % BLK
            blocks[0] = jnp.where(keys_at <= query_at, blocks[0], NEGATIVE)
        peak = None if old is None else old[0]
        for block, neg in zip(blocks, negs):
            high = jnp.max(block, axis=0, keepdims=True) * SCALE + neg
            peak = high if peak is None else jnp.maximum(peak, high)
        weights = [jnp.exp2(block * SCALE - (peak - neg)) for block, neg in zip(blocks, negs)]
        amount = None
        for w in weights:
            part = jnp.sum(w, axis=0, keepdims=True)
            amount = part if amount is None else amount + part
        p = jnp.concatenate([w.astype(jnp.bfloat16) for w in weights], axis=0)
        mix = jnp.dot(vt, p, preferred_element_type=jnp.float32)
        if old is not None:
            shrink = jnp.exp2(old[0] - peak)
            amount = amount + old[1] * shrink
            mix = mix + old[2] * shrink
        return peak, amount, mix

    def keep(a, state):
        top[a], total[a], acc[a] = state

    def before(a):
        return top[a], total[a], acc[a]

    def near(slab):
        done = []
        for i in range(slab_blocks):
            a = slab * slab_blocks + i
            ks, vs, negs = [kbuf[a]], [vbuf[a]], [jnp.float32(0)]
            for j in range(slashes):
                at = a - slash_ref[j, c]
                here = jnp.maximum(at, 0)
                ks.append(kbuf[here])
                vs.append(vbuf[here])
                negs.append(jnp.where(at >= 0, 0.0, NEGATIVE))
            state = update(a, jnp.concatenate(ks, axis=0), jnp.concatenate(vs, axis=0).T, negs,
                           None, True)
            done.append((a, state))
        for a, state in done:
            keep(a, state)

    def far_negs(a, g, count):
        negs = []
        for i in range(count * grain):
            gap = first + a - vert_ref[c, g * grain + i]
            negs.append(jnp.where((gap > 0) & jnp.logical_not(on_slash(gap)), 0.0, NEGATIVE))
        return negs

    def far_keys(g, count):
        return jnp.concatenate([pos[g * grain + i, :BLK] for i in range(count * grain)], axis=0)

    def far_values(g, count):
        return jnp.concatenate([vtpos[g + i] for i in range(count)], axis=1)

    def far(slab, g, count):
        done = []
        for i in range(slab_blocks):
            a = slab * slab_blocks + i
            done.append((a, update(a, far_keys(g, count), far_values(g, count),
                                   far_negs(a, g, count), before(a))))
        for a, state in done:
            keep(a, state)

    def back(_):
        k = jnp.concatenate([prev[0, i] for i in range(slab_blocks)], axis=0)
        vt = jnp.concatenate([prev[1, i] for i in range(slab_blocks)], axis=0).T
        done = []
        for a in range(slab_blocks):
            negs = []
            for i in range(slab_blocks):
                hit = on_slash(a + slab_blocks - i)
                negs.append(jnp.where(hit, 0.0, NEGATIVE))
            done.append((a, update(a, k, vt, negs, before(a))))
        for a, state in done:
            keep(a, state)

    def finish(slab, e):
        done = []
        for i in range(slab_blocks):
            a = slab * slab_blocks + i
            done.append(update(a, far_keys(0, 1), far_values(0, 1), far_negs(a, 0, 1), before(a)))
        for i, (_, amount, mix) in enumerate(done):
            out = (mix * (1.0 / amount)).T.astype(abuf.dtype)
            for g in range(per_group):
                abuf[e, i * BLK:(i + 1) * BLK, g * HEAD_DIM:(g + 1) * HEAD_DIM] = (
                    out[g * BLK:(g + 1) * BLK])

    own_copies[0].wait()
    own_copies[1].wait()
    for e in others:
        handed(k_hbm, kbuf, HEAD_DIM, k_send.at[e], k_recv, c, source(e)).wait_recv()
        handed(v_hbm, vbuf, HEAD_DIM, v_send.at[e], v_recv, c, source(e)).wait_recv()

    @pl.when((o == outer - 2))
    def _():
        start_prev()

    own_copies[2].wait()

    def early(i, _):
        g = grains - 1 - i

        @pl.when(o < outer - 1)
        def _():
            chain(g)

        return 0

    lax.fori_loop(0, grains - 1, early, 0)
    near(c)

    def gather(i, _):
        e = inner - 1 - i
        slab = source(e)
        handed(q_hbm, qbuf, width, q_send.at[e], q_recv, c, slab).wait_recv()
        near(slab)
        return 0

    lax.fori_loop(0, inner - 1, gather, 0)

    @pl.when(o < outer - 1)
    def _():
        chain(0)

    @pl.when(o < outer - 2)
    def _():
        start_prev()

    def mid(i, _):
        g = grains - (i + 1) * middle

        @pl.when(o == outer - 1)
        def _():
            for j in range(middle):
                chain(g + middle - 1 - j)

        lax.fori_loop(0, inner, lambda slab, z: (far(slab, g, middle), z)[1], 0)
        return 0

    lax.fori_loop(0, (grains - 1) // middle, mid, 0)

    @pl.when(o > 0)
    def _():
        for part in range(2):
            prev_copy(part).wait_recv()
        back(0)

    @pl.when(o == outer - 1)
    def _():
        chain(0)

    def return_copy(e):
        return remote(abuf.at[e], attn.at[c], r_send.at[e], r_recv.at[c], base + source(e))

    def last(i, _):
        e = inner - 1 - i
        finish(source(e), e)

        @pl.when(e > 0)
        def _():
            return_copy(e).start()

        return 0

    lax.fori_loop(0, inner, last, 0)

    weight_copy.wait()
    tiles = give.shape[0]
    mine = pl.ds(pl.multiple_of(core * half, half), half)
    theirs = pl.ds(pl.multiple_of(other * half, half), half)

    def columns(t):
        return pl.ds(pl.multiple_of(t * tile, tile), tile)

    def swap(t):
        return pltpu.make_async_remote_copy(
            src_ref=give.at[t], dst_ref=take.at[t], send_sem=x_send.at[t], recv_sem=x_recv.at[t],
            device_id=(me, other), device_id_type=MESH,
        )

    def product(values, h, t):
        return jnp.dot(values, w_ref[span(h, width), columns(t)],
                       preferred_element_type=jnp.float32)

    def project_own(t, _):
        res[t] = product(abuf[0], c, t)
        return 0

    lax.fori_loop(0, tiles, project_own, 0)

    def returned(e):
        h = peer(e)
        remote(abuf.at[e], attn.at[h], r_send.at[e], r_recv.at[h], above).wait_recv()
        return h

    for e in others[:-1]:
        h = returned(e)

        def project_more(t, _, h=h):
            res[t] = res[t] + product(attn[h], h, t)
            return 0

        lax.fori_loop(0, tiles, project_more, 0)

    h_last = returned(others[-1])

    def project_last(t, _):
        out = res[t] + product(attn[h_last], h_last, t)
        res[t] = out
        give[t] = res[t, theirs, :].astype(jnp.bfloat16)
        swap(t).start()
        return 0

    lax.fori_loop(0, tiles, project_last, 0)

    def add_up(t, _):
        swap(t).wait_recv()
        out_ref[:, columns(t)] = (res[t, mine, :] + take[t].astype(jnp.float32)).astype(out_ref.dtype)
        return 0

    lax.fori_loop(0, tiles, add_up, 0)

    def sent(t, _):
        swap(t).wait_send()
        return 0

    lax.fori_loop(0, tiles, sent, 0)
    for e in others:
        give_k(e).wait_send()
        give_v(e).wait_send()
        give_q(e).wait_send()
        return_copy(e).wait_send()

    @pl.when(o < outer - 1)
    def _():
        for part in range(2):
            prev_copy(part).wait_send()

    def left(g, _):
        @pl.when(leaving(g))
        def _():
            chain_copy(g).wait_send()

        return 0

    lax.fori_loop(0, grains, left, 0)


def on_device(n, queries, keys, values, vertical, slash, out_weight):
    rows = queries.shape[0]
    inner = vertical.shape[0]
    per_group = queries.shape[1] // (inner * HEAD_DIM)
    width = per_group * HEAD_DIM
    slab_blocks = rows // BLK
    plane_blocks = inner * slab_blocks
    chosen = vertical.shape[1]
    model = out_weight.shape[1]
    grain = math.gcd(chosen, 4)
    grains = chosen // grain
    middle = 3 if (grains - 1) % 3 == 0 else 1
    tile = math.gcd(model, 512)
    tiles = model // tile
    bf16, f32 = jnp.bfloat16, jnp.float32
    vmem = pl.BlockSpec(memory_space=pltpu.VMEM)
    smem = pl.BlockSpec(memory_space=pltpu.SMEM)
    hbm = pl.BlockSpec(memory_space=pl.ANY)
    dma = pltpu.SemaphoreType.DMA
    return pl.pallas_call(
        functools.partial(kernel, n, inner, per_group, tile, grain, middle),
        out_shape=jax.ShapeDtypeStruct((rows // 2, model), bf16),
        in_specs=[hbm] * 3 + [smem] * 2 + [hbm],
        out_specs=vmem,
        scratch_shapes=[
            pltpu.VMEM((plane_blocks, BLK, width), bf16),
            pltpu.VMEM((plane_blocks, BLK, HEAD_DIM), bf16),
            pltpu.VMEM((plane_blocks, BLK, HEAD_DIM), bf16),
            pltpu.VMEM((2, slab_blocks, BLK, HEAD_DIM), bf16),
            pltpu.VMEM((chosen, 2 * BLK, HEAD_DIM), bf16),
            pltpu.VMEM((chosen, 2 * BLK, HEAD_DIM), bf16),
            pltpu.VMEM((grains, HEAD_DIM, grain * BLK), bf16),
            pltpu.VMEM((plane_blocks, HEAD_DIM, per_group * BLK), f32),
            pltpu.VMEM((plane_blocks, 1, per_group * BLK), f32),
            pltpu.VMEM((plane_blocks, 1, per_group * BLK), f32),
            pltpu.VMEM((inner, rows, width), bf16),
            pltpu.VMEM((inner, rows, width), bf16),
            pltpu.VMEM(out_weight.shape, bf16),
            pltpu.VMEM((tiles, rows, tile), f32),
            pltpu.VMEM((tiles, rows // 2, tile), bf16),
            pltpu.VMEM((tiles, rows // 2, tile), bf16),
            dma((3,)),
            dma,
            dma((inner,)), dma((inner,)),
            dma((inner,)), dma((inner,)),
            dma((inner,)), dma((inner,)),
            dma((2,)), dma((2,)),
            dma((grains,)), dma((grains,)),
            dma((inner,)), dma((inner,)),
            dma((tiles,)), dma((tiles,)),
        ],
        compiler_params=pltpu.CompilerParams(
            collective_id=0, has_side_effects=True, vmem_limit_bytes=60 * 2**20
        ),
    )(*(x.reshape(slab_blocks, BLK, -1) for x in (queries, keys, values)),
      vertical, slash.T, out_weight)


def solution(mesh):
    placed = (
        P("seq", "head"),
        P("seq", "head"),
        P("seq", "head"),
        P("head", None),
        P("head", None),
        P("head", None),
    )
    return jax.shard_map(
        functools.partial(on_device, mesh.shape["seq"]),
        mesh=mesh, in_specs=placed, out_specs=P(("seq", "head"), None), check_vma=False,
    )
```

```python
import functools
import math

import jax
import jax.numpy as jnp
from jax import lax
from jax.experimental import pallas as pl
from jax.experimental.pallas import tpu as pltpu
from jax.sharding import PartitionSpec as P

HEAD_DIM = 128
BLK = 64
CAP = 2
FAR = 4
UNROLL = 4
NEGATIVE = -1e30
MESH = pl.DeviceIdType.MESH
SCALE = HEAD_DIM ** (-0.5) * math.log2(math.e)


def kernel(
    n, inner, per_group, tile, grain, group,
    q_hbm, k_hbm, v_hbm, vert_ref, slash_ref, w_hbm, out_ref,
    kloc, vloc, pack, sel, qbuf, kbuf, vbuf, prev, inc, pos, vtpos, acc, top, total, abuf, attn, w_ref, res, give, take,
    local_sem, w_sem, s_send, s_recv, k_send, k_recv, v_send, v_recv, q_send, q_recv,
    p_send, p_recv, c_send, c_recv, r_send, r_recv, x_send, x_recv,
):
    slab_blocks = q_hbm.shape[0]
    rows = slab_blocks * BLK
    width = per_group * HEAD_DIM
    outer = n // inner
    me = lax.axis_index("seq")
    core = lax.axis_index("head")
    o, c = me // inner, me % inner
    other = 1 - core
    plane_blocks = inner * slab_blocks
    first = o * plane_blocks
    chosen = vert_ref.shape[1]
    grains = chosen // grain
    slashes = slash_ref.shape[0]
    half = rows // 2
    base = o * inner
    pair = math.gcd(inner, 2)

    def peer(e):
        return ((c // pair + e // pair) % (inner // pair)) * pair + (c % pair + e % pair) % pair

    def source(e):
        up = (c // pair + inner // pair - e // pair) % (inner // pair)
        return up * pair + (c % pair + pair - e % pair) % pair

    barrier = pltpu.get_barrier_semaphore()

    def greet(seq, head):
        pl.semaphore_signal(barrier, inc=1, device_id=(seq, head), device_id_type=MESH)

    greet(me, other)
    for e in range(1, inner):
        greet(base + peer(e), core)

    @pl.when(o < outer - 1)
    def _():
        greet(me + inner, core)

    @pl.when(o > 0)
    def _():
        greet(me - inner, core)

    def span(index, size):
        return pl.ds(pl.multiple_of(index * size, size), size)

    loads = [pltpu.make_async_copy(k_hbm, kloc, local_sem.at[3]),
             pltpu.make_async_copy(v_hbm, vloc, local_sem.at[4])]
    for copy in loads:
        copy.start()
    own_copies = [
        pltpu.make_async_copy(hbm.at[:, :, span(c, size)], ref.at[span(c, slab_blocks)], local_sem.at[i])
        for i, (hbm, ref, size) in enumerate(
            ((k_hbm, kbuf, HEAD_DIM), (v_hbm, vbuf, HEAD_DIM), (q_hbm, qbuf, width)))
    ]
    for copy in own_copies:
        copy.start()

    def remote(src, dst, send_sem, recv_sem, seq):
        return pltpu.make_async_remote_copy(
            src_ref=src, dst_ref=dst, send_sem=send_sem, recv_sem=recv_sem,
            device_id=(seq, core), device_id_type=MESH,
        )

    def handed(hbm, ref, size, send_sem, recv_sem, to, slab):
        return remote(hbm.at[:, :, span(to, size)], ref.at[span(slab, slab_blocks)], send_sem,
                      recv_sem.at[slab], base + to)

    def give_k(e):
        return handed(k_hbm, kbuf, HEAD_DIM, k_send.at[e], k_recv, peer(e), c)

    def give_v(e):
        return handed(v_hbm, vbuf, HEAD_DIM, v_send.at[e], v_recv, peer(e), c)

    def give_q(e):
        return handed(q_hbm, qbuf, width, q_send.at[e], q_recv, peer(e), c)

    others = range(inner - 1, 0, -1)
    for copy in loads:
        copy.wait()
    for h in range(inner):
        low, high = jnp.int32(slab_blocks), jnp.int32(-1)
        for i in range(chosen):
            block = vert_ref[h, i] - me * slab_blocks
            inside = (block >= 0) & (block < slab_blocks)
            low = jnp.where(inside, jnp.minimum(low, block), low)
            high = jnp.where(inside, jnp.maximum(high, block), high)
        lanes = slice(h * HEAD_DIM, (h + 1) * HEAD_DIM)
        for slot, block in enumerate((jnp.minimum(low, slab_blocks - 1), jnp.maximum(high, 0))):
            pack[h, slot, :BLK] = kloc[block, :, lanes]
            pack[h, slot, BLK:] = vloc[block, :, lanes]

    pl.semaphore_wait(
        barrier, inner + jnp.where(o > 0, 1, 0) + jnp.where(o < outer - 1, 1, 0))

    def give_sel(e):
        return remote(pack.at[peer(e)], sel.at[span(c, CAP)], s_send.at[e], s_recv.at[c],
                      base + peer(e))

    for e in others:
        give_sel(e).start()
    for e in others:
        give_k(e).start()
        give_v(e).start()
    for e in others:
        give_q(e).start()
    weight_copy = pltpu.make_async_copy(w_hbm, w_ref, w_sem)
    weight_copy.start()
    for slot in range(CAP):
        sel[c * CAP + slot] = pack[c, slot]

    above = (me + inner) % n

    def chain_copy(g):
        there = pl.ds(pl.multiple_of(g * grain, grain), grain)
        return remote(pos.at[there], inc.at[there], c_send.at[g], c_recv.at[g], above)

    def prev_copy(part):
        ref = (kbuf, vbuf)[part]
        return remote(ref.at[span(inner - 1, slab_blocks)], prev.at[part], p_send.at[part],
                      p_recv.at[part], above)

    def arriving(g):
        return g * grain < CAP * inner * o

    def leaving(g):
        return (o < outer - 1) & (g * grain < CAP * inner * (o + 1))

    def chain(g):
        @pl.when(arriving(g))
        def _():
            chain_copy(g).wait_recv()

        @pl.when(jnp.logical_not(arriving(g)))
        def _():
            there = pl.ds(pl.multiple_of(g * grain, grain), grain)
            inc[there] = jnp.zeros((grain, 2 * BLK, HEAD_DIM), inc.dtype)

        picked = []
        for i in range(grain):
            p = g * grain + i
            at = vert_ref[c, p] - first
            mine = (at >= 0) & (at < plane_blocks)
            slab = jnp.clip(at, 0, plane_blocks - 1) // slab_blocks
            below = vert_ref[c, jnp.maximum(p - 1, 0)] - first
            second = (p > 0) & (below >= slab * slab_blocks) & (below < at)
            both = jnp.where(mine, sel[slab * CAP + jnp.where(second, 1, 0)], inc[p])
            pos[p] = both
            picked.append(both[BLK:])

        @pl.when(leaving(g))
        def _():
            chain_copy(g).start()

        vtpos[g] = jnp.concatenate(picked, axis=0).T

    def start_prev():
        for part in range(2):
            prev_copy(part).start()

    def queries(a):
        return jnp.concatenate(
            [qbuf[a, :, g * HEAD_DIM:(g + 1) * HEAD_DIM] for g in range(per_group)], axis=0)

    def on_slash(gap):
        hit = gap == slash_ref[0, c]
        for i in range(1, slashes):
            hit = hit | (gap == slash_ref[i, c])
        return hit

    def fold(block, op):
        parts = [block[i * 8:(i + 1) * 8] for i in range(BLK // 8)]
        while len(parts) > 1:
            parts = [op(x, y) for x, y in zip(parts[::2], parts[1::2])]
        return parts[0]

    def scores_of(a, k, triangle=False):
        s = lax.dot_general(k, queries(a), (((1,), (1,)), ((), ())),
                            preferred_element_type=jnp.float32)
        blocks = [s[i * BLK:(i + 1) * BLK] for i in range(k.shape[0] // BLK)]
        if triangle:
            keys_at = lax.broadcasted_iota(jnp.int32, blocks[0].shape, 0)
            query_at = lax.broadcasted_iota(jnp.int32, blocks[0].shape, 1) % BLK
            blocks[0] = jnp.where(keys_at <= query_at, blocks[0], NEGATIVE)
        return blocks

    def weigh(blocks, negs, old):
        high = None
        for block, neg in zip(blocks, negs):
            part = fold(block, jnp.maximum)
            part = part if neg is None else part + neg
            high = part if high is None else jnp.maximum(high, part)
        peak = jnp.max(high, axis=0, keepdims=True) * SCALE
        if old is not None:
            peak = jnp.maximum(peak, old[0])
        amount, packed = None, []
        for block, neg in zip(blocks, negs):
            w = jnp.exp2(block * SCALE - (peak if neg is None else peak - neg))
            part = fold(w, jnp.add)
            amount = part if amount is None else amount + part
            packed.append(w.astype(jnp.bfloat16))
        shrink = None
        if old is not None:
            shrink = jnp.exp2(old[0] - peak)
            amount = amount + old[1] * shrink
        return peak, amount, shrink, jnp.concatenate(packed, axis=0)

    def attend(todo, old, triangle=False):
        scores = [scores_of(a, k, triangle) for a, k, _, _ in todo]
        soft = [weigh(blocks, negs, before(a) if old else None)
                for blocks, (a, _, _, negs) in zip(scores, todo)]
        done = []
        for (peak, amount, shrink, p), (a, _, vt, _) in zip(soft, todo):
            mix = jnp.dot(vt, p, preferred_element_type=jnp.float32)
            if old:
                mix = mix + acc[a] * shrink
            done.append((peak, amount, mix))
        return done

    def before(a):
        return top[a], total[a]

    def keep(todo, done):
        for (a, _, _, _), state in zip(todo, done):
            top[a], total[a], acc[a] = state

    def near(slab):
        todo = []
        for i in range(slab_blocks):
            a = slab * slab_blocks + i
            ks, vs, negs = [kbuf[a]], [vbuf[a]], [None]
            for j in range(slashes):
                at = a - slash_ref[j, c]
                here = jnp.maximum(at, 0)
                ks.append(kbuf[here])
                vs.append(vbuf[here])
                negs.append(jnp.where(at >= 0, 0.0, NEGATIVE))
            todo.append((a, jnp.concatenate(ks, axis=0), jnp.concatenate(vs, axis=0).T, negs))
        keep(todo, attend(todo, False, True))

    def on_far(a, g, count):
        negs = []
        for i in range(count * grain):
            gap = first + a - vert_ref[c, g * grain + i]
            negs.append(jnp.where((gap > 0) & jnp.logical_not(on_slash(gap)), 0.0, NEGATIVE))
        k = jnp.concatenate([pos[g * grain + i, :BLK] for i in range(count * grain)], axis=0)
        vt = jnp.concatenate([vtpos[g + i] for i in range(count)], axis=1)
        return a, k, vt, negs

    def far(slab, g, count):
        for part in range(0, slab_blocks, FAR):
            todo = [on_far(slab * slab_blocks + part + i, g, count) for i in range(FAR)]
            keep(todo, attend(todo, True))

    def back(_):
        k = jnp.concatenate([prev[0, i] for i in range(slab_blocks)], axis=0)
        vt = jnp.concatenate([prev[1, i] for i in range(slab_blocks)], axis=0).T
        todo = []
        for a in range(slab_blocks):
            negs = [jnp.where(on_slash(a + slab_blocks - i), 0.0, NEGATIVE)
                    for i in range(slab_blocks)]
            todo.append((a, k, vt, negs))
        keep(todo, attend(todo, True))

    def finish(slab, e):
        done = []
        for part in range(0, slab_blocks, FAR):
            done += attend([on_far(slab * slab_blocks + part + i, 0, group)
                            for i in range(FAR)], True)
        for i, (_, amount, mix) in enumerate(done):
            amount = jnp.sum(amount, axis=0, keepdims=True)
            out = (mix * (1.0 / amount)).astype(abuf.dtype).T
            for g in range(per_group):
                abuf[e, i * BLK:(i + 1) * BLK, g * HEAD_DIM:(g + 1) * HEAD_DIM] = (
                    out[g * BLK:(g + 1) * BLK])

    for e in others:
        slab = source(e)
        remote(pack.at[c], sel.at[span(slab, CAP)], s_send.at[e], s_recv.at[slab], above).wait_recv()

    @pl.when(o < outer - 1)
    def _():
        lax.fori_loop(0, grains, lambda i, z: (chain(grains - 1 - i), z)[1], 0)

    own_copies[0].wait()
    own_copies[1].wait()
    for e in others:
        handed(k_hbm, kbuf, HEAD_DIM, k_send.at[e], k_recv, c, source(e)).wait_recv()
        handed(v_hbm, vbuf, HEAD_DIM, v_send.at[e], v_recv, c, source(e)).wait_recv()

    @pl.when(o < outer - 1)
    def _():
        start_prev()

    own_copies[2].wait()

    near(c)

    def return_copy(e):
        return remote(abuf.at[e], attn.at[c], r_send.at[e], r_recv.at[c], base + source(e))

    def last(i, _):
        e = inner - 1 - i
        slab = source(e)

        @pl.when(e > 0)
        def _():
            handed(q_hbm, qbuf, width, q_send.at[e], q_recv, c, slab).wait_recv()
            near(slab)

        @pl.when((i == 0) & (o == outer - 1))
        def _():
            lax.fori_loop(0, grains, lambda i, z: (chain(grains - 1 - i), z)[1], 0)

        @pl.when((slab == 0) & (o > 0))
        def _():
            for part in range(2):
                prev_copy(part).wait_recv()
            back(0)

        lax.fori_loop(0, grains // group - 1,
                      lambda i, z: (far(slab, grains - (i + 1) * group, group), z)[1], 0)
        finish(slab, e)

        @pl.when(e > 0)
        def _():
            return_copy(e).start()

        return 0

    lax.fori_loop(0, inner, last, 0)

    weight_copy.wait()
    tiles = give.shape[0]
    mine = pl.ds(pl.multiple_of(core * half, half), half)
    theirs = pl.ds(pl.multiple_of(other * half, half), half)

    def columns(t):
        return pl.ds(pl.multiple_of(t * tile, tile), tile)

    def swap(t):
        return pltpu.make_async_remote_copy(
            src_ref=give.at[t], dst_ref=take.at[t], send_sem=x_send.at[t], recv_sem=x_recv.at[t],
            device_id=(me, other), device_id_type=MESH,
        )

    def product(values, h, t):
        return jnp.dot(values, w_ref[span(h, width), columns(t)],
                       preferred_element_type=jnp.float32)

    def project_own(t, _):
        res[t] = product(abuf[0], c, t)
        return 0

    lax.fori_loop(0, tiles, project_own, 0, unroll=UNROLL)

    def returned(e):
        h = peer(e)
        remote(abuf.at[e], attn.at[h], r_send.at[e], r_recv.at[h], above).wait_recv()
        return h

    for e in others[:-1]:
        h = returned(e)

        def project_more(t, _, h=h):
            res[t] = res[t] + product(attn[h], h, t)
            return 0

        lax.fori_loop(0, tiles, project_more, 0, unroll=UNROLL)

    h_last = returned(others[-1])

    def project_last(t, _):
        out = res[t] + product(attn[h_last], h_last, t)
        res[t] = out
        give[t] = res[t, theirs, :].astype(jnp.bfloat16)
        swap(t).start()
        return 0

    lax.fori_loop(0, tiles, project_last, 0, unroll=UNROLL)

    def add_up(t, _):
        swap(t).wait_recv()
        out_ref[:, columns(t)] = (res[t, mine, :] + take[t].astype(jnp.float32)).astype(out_ref.dtype)
        return 0

    lax.fori_loop(0, tiles, add_up, 0)

    def sent(t, _):
        swap(t).wait_send()
        return 0

    lax.fori_loop(0, tiles, sent, 0)
    for e in others:
        give_sel(e).wait_send()
        give_k(e).wait_send()
        give_v(e).wait_send()
        give_q(e).wait_send()
        return_copy(e).wait_send()

    @pl.when(o < outer - 1)
    def _():
        for part in range(2):
            prev_copy(part).wait_send()

    def left(g, _):
        @pl.when(leaving(g))
        def _():
            chain_copy(g).wait_send()

        return 0

    lax.fori_loop(0, grains, left, 0)


def on_device(n, queries, keys, values, vertical, slash, out_weight):
    rows = queries.shape[0]
    inner = vertical.shape[0]
    per_group = queries.shape[1] // (inner * HEAD_DIM)
    width = per_group * HEAD_DIM
    slab_blocks = rows // BLK
    plane_blocks = inner * slab_blocks
    chosen = vertical.shape[1]
    model = out_weight.shape[1]
    grain = math.gcd(chosen, 4)
    grains = chosen // grain
    group = math.gcd(grains, 4)
    tile = math.gcd(model, 512)
    tiles = model // tile
    bf16, f32 = jnp.bfloat16, jnp.float32
    vmem = pl.BlockSpec(memory_space=pltpu.VMEM)
    smem = pl.BlockSpec(memory_space=pltpu.SMEM)
    hbm = pl.BlockSpec(memory_space=pl.ANY)
    dma = pltpu.SemaphoreType.DMA
    return pl.pallas_call(
        functools.partial(kernel, n, inner, per_group, tile, grain, group),
        out_shape=pltpu.VMEM((rows // 2, model), bf16),
        in_specs=[hbm] * 3 + [smem] * 2 + [hbm],
        out_specs=vmem,
        scratch_shapes=[
            pltpu.VMEM((slab_blocks, BLK, inner * HEAD_DIM), bf16),
            pltpu.VMEM((slab_blocks, BLK, inner * HEAD_DIM), bf16),
            pltpu.VMEM((inner, CAP, 2 * BLK, HEAD_DIM), bf16),
            pltpu.VMEM((inner * CAP, 2 * BLK, HEAD_DIM), bf16),
            pltpu.VMEM((plane_blocks, BLK, width), bf16),
            pltpu.VMEM((plane_blocks, BLK, HEAD_DIM), bf16),
            pltpu.VMEM((plane_blocks, BLK, HEAD_DIM), bf16),
            pltpu.VMEM((2, slab_blocks, BLK, HEAD_DIM), bf16),
            pltpu.VMEM((chosen, 2 * BLK, HEAD_DIM), bf16),
            pltpu.VMEM((chosen, 2 * BLK, HEAD_DIM), bf16),
            pltpu.VMEM((grains, HEAD_DIM, grain * BLK), bf16),
            pltpu.VMEM((plane_blocks, HEAD_DIM, per_group * BLK), f32),
            pltpu.VMEM((plane_blocks, 1, per_group * BLK), f32),
            pltpu.VMEM((plane_blocks, 8, per_group * BLK), f32),
            pltpu.VMEM((inner, rows, width), bf16),
            pltpu.VMEM((inner, rows, width), bf16),
            pltpu.VMEM(out_weight.shape, bf16),
            pltpu.VMEM((tiles, rows, tile), f32),
            pltpu.VMEM((tiles, rows // 2, tile), bf16),
            pltpu.VMEM((tiles, rows // 2, tile), bf16),
            dma((5,)),
            dma,
            dma((inner,)), dma((inner,)),
            dma((inner,)), dma((inner,)),
            dma((inner,)), dma((inner,)),
            dma((inner,)), dma((inner,)),
            dma((2,)), dma((2,)),
            dma((grains,)), dma((grains,)),
            dma((inner,)), dma((inner,)),
            dma((tiles,)), dma((tiles,)),
        ],
        compiler_params=pltpu.CompilerParams(
            collective_id=0, has_side_effects=True, vmem_limit_bytes=60 * 2**20
        ),
    )(*(x.reshape(slab_blocks, BLK, -1) for x in (queries, keys, values)),
      vertical, slash.T, out_weight)


def solution(mesh):
    placed = (
        P("seq", "head"),
        P("seq", "head"),
        P("seq", "head"),
        P("head", None),
        P("head", None),
        P("head", None),
    )
    return jax.shard_map(
        functools.partial(on_device, mesh.shape["seq"]),
        mesh=mesh, in_specs=placed, out_specs=P(("seq", "head"), None), check_vma=False,
    )
```

```python
import functools
import math

import jax
import jax.numpy as jnp
from jax import lax
from jax.experimental import pallas as pl
from jax.experimental.pallas import tpu as pltpu
from jax.sharding import PartitionSpec as P

HEAD_DIM = 128
BLK = 64
CAP = 2
FAR = 4
UNROLL = 4
NEGATIVE = -1e30
MESH = pl.DeviceIdType.MESH
SCALE = HEAD_DIM ** (-0.5) * math.log2(math.e)


def kernel(
    n, inner, per_group, tile, grain, group, split,
    q_hbm, k_hbm, v_hbm, vert_ref, slash_ref, w_hbm, out_ref,
    kloc, vloc, pack, sel, rest, slots, qbuf, prev, inc, pos, vtpos, acc, top, total, abuf, attn, w_ref, res, give, take,
    local_sem, w_sem, s_send, s_recv, k_send, k_recv, q_send, q_recv,
    p_send, p_recv, c_send, c_recv, r_send, r_recv, x_send, x_recv, turn,
):
    slab_blocks = q_hbm.shape[0]
    rows = slab_blocks * BLK
    width = per_group * HEAD_DIM
    outer = n // inner
    me = lax.axis_index("seq")
    core = lax.axis_index("head")
    o, c = me // inner, me % inner
    other = 1 - core
    plane_blocks = inner * slab_blocks
    first = o * plane_blocks
    chosen = vert_ref.shape[1]
    grains = chosen // grain
    slashes = slash_ref.shape[0]
    base = o * inner
    pair = math.gcd(inner, 2)

    def peer(e):
        return ((c // pair + e // pair) % (inner // pair)) * pair + (c % pair + e % pair) % pair

    def source(e):
        up = (c // pair + inner // pair - e // pair) % (inner // pair)
        return up * pair + (c % pair + pair - e % pair) % pair

    barrier = pltpu.get_barrier_semaphore()

    def greet(seq, head):
        pl.semaphore_signal(barrier, inc=1, device_id=(seq, head), device_id_type=MESH)

    greet(me, other)
    for e in range(1, inner):
        greet(base + peer(e), core)

    @pl.when(o < outer - 1)
    def _():
        greet(me + inner, core)

    @pl.when(o > 0)
    def _():
        greet(me - inner, core)

    def span(index, size):
        return pl.ds(pl.multiple_of(index * size, size), size)

    loads = [
        pltpu.make_async_copy(k_hbm, kloc, local_sem.at[0]),
        pltpu.make_async_copy(v_hbm, vloc, local_sem.at[1]),
        pltpu.make_async_copy(q_hbm.at[:, :, span(c, width)], qbuf.at[span(c, slab_blocks)],
                              local_sem.at[2]),
    ]
    for copy in loads:
        copy.start()

    def remote(src, dst, send_sem, recv_sem, seq):
        return pltpu.make_async_remote_copy(
            src_ref=src, dst_ref=dst, send_sem=send_sem, recv_sem=recv_sem,
            device_id=(seq, core), device_id_type=MESH,
        )

    others_count = slab_blocks - CAP

    def give_sel(e, to, slab):
        return remote(pack.at[to, :CAP], sel.at[span(slab, CAP)], s_send.at[e],
                      s_recv.at[slab], base + to)

    def give_rest(e, to, slab):
        return remote(pack.at[to, CAP:], rest.at[span(slab, others_count)], k_send.at[e],
                      k_recv.at[slab], base + to)

    def give_q(e, to, slab):
        return remote(q_hbm.at[:, :, span(to, width)], qbuf.at[span(slab, slab_blocks)],
                      q_send.at[e], q_recv.at[slab], base + to)

    others = range(inner - 1, 0, -1)
    loads[0].wait()
    loads[1].wait()

    def order(h, slab):
        low, high = jnp.int32(slab_blocks), jnp.int32(-1)
        for i in range(chosen):
            block = vert_ref[h, i] - slab * slab_blocks
            inside = (block >= 0) & (block < slab_blocks)
            low = jnp.where(inside, jnp.minimum(low, block), low)
            high = jnp.where(inside, jnp.maximum(high, block), high)
        low = jnp.where(high < 0, 0, low)
        high = jnp.where(high > low, high, jnp.where(low == 0, 1, 0))
        ranks, left = [], jnp.int32(CAP)
        for j in range(slab_blocks):
            taken = (low == j) | (high == j)
            ranks.append(jnp.where(low == j, 0, jnp.where(high == j, 1, left)))
            left = jnp.where(taken, left, left + 1)
        blocks = []
        for i in range(slab_blocks):
            at = jnp.int32(0)
            for j in range(1, slab_blocks):
                at = jnp.where(ranks[j] == i, j, at)
            blocks.append(at)
        return ranks, blocks

    for h in range(inner):
        lanes = slice(h * HEAD_DIM, (h + 1) * HEAD_DIM)
        for i, block in enumerate(order(h, me)[1]):
            pack[h, i, :BLK] = kloc[block, :, lanes]
            pack[h, i, BLK:] = vloc[block, :, lanes]

    pl.semaphore_wait(
        barrier, inner + jnp.where(o > 0, 1, 0) + jnp.where(o < outer - 1, 1, 0))

    for e in others:
        give_sel(e, peer(e), c).start()

    for e in others:
        give_rest(e, peer(e), c).start()

    for e in others:
        give_q(e, peer(e), c).start()
    weight_copy = pltpu.make_async_copy(w_hbm, w_ref, w_sem)
    weight_copy.start()
    for i in range(slab_blocks):
        if i < CAP:
            sel[c * CAP + i] = pack[c, i]
        else:
            rest[c * others_count + i - CAP] = pack[c, i]
    for slab in range(inner):
        for j, rank in enumerate(order(c, base + slab)[0]):
            slots[slab * slab_blocks + j] = rank
    prev_blocks = order(c, base - 1)[1]

    above = (me + inner) % n

    def chain_copy(g):
        there = pl.ds(pl.multiple_of(g * grain, grain), grain)
        return remote(pos.at[there], inc.at[there], c_send.at[g], c_recv.at[g], above)

    def prev_copy(part):
        if part:
            source_ref, there = rest.at[span(inner - 1, others_count)], prev.at[CAP:]
        else:
            source_ref, there = sel.at[span(inner - 1, CAP)], prev.at[:CAP]
        return remote(source_ref, there, p_send.at[part], p_recv.at[part], above)

    def arriving(g):
        return g * grain < CAP * inner * o

    def leaving(g):
        return (o < outer - 1) & (g * grain < CAP * inner * (o + 1))

    def chain(g):
        @pl.when(arriving(g))
        def _():
            chain_copy(g).wait_recv()

        @pl.when(jnp.logical_not(arriving(g)))
        def _():
            there = pl.ds(pl.multiple_of(g * grain, grain), grain)
            inc[there] = jnp.zeros((grain, 2 * BLK, HEAD_DIM), inc.dtype)

        picked = []
        for i in range(grain):
            p = g * grain + i
            at = vert_ref[c, p] - first
            mine = (at >= 0) & (at < plane_blocks)
            slab = jnp.clip(at, 0, plane_blocks - 1) // slab_blocks
            below = vert_ref[c, jnp.maximum(p - 1, 0)] - first
            second = (p > 0) & (below >= slab * slab_blocks) & (below < at)
            both = jnp.where(mine, sel[slab * CAP + jnp.where(second, 1, 0)], inc[p])
            pos[p] = both
            picked.append(both[BLK:])

        @pl.when((core == 0) & (o < outer - 1) & (g == grains - 1))
        def _():
            pl.semaphore_wait(turn, 1)

        @pl.when(leaving(g))
        def _():
            chain_copy(g).start()

        @pl.when((core == 1) & (o < outer - 1) & (g == 0))
        def _():
            pl.semaphore_signal(turn, inc=1, device_id=(me, 0), device_id_type=MESH)

        vtpos[g] = jnp.concatenate(picked, axis=0).T

    def start_prev():
        for part in range(2):
            prev_copy(part).start()

    def queries(a):
        return jnp.concatenate(
            [qbuf[a, :, g * HEAD_DIM:(g + 1) * HEAD_DIM] for g in range(per_group)], axis=0)

    def on_slash(gap):
        hit = gap == slash_ref[0, c]
        for i in range(1, slashes):
            hit = hit | (gap == slash_ref[i, c])
        return hit

    def fold(block, op):
        parts = [block[i * 8:(i + 1) * 8] for i in range(BLK // 8)]
        while len(parts) > 1:
            parts = [op(x, y) for x, y in zip(parts[::2], parts[1::2])]
        return parts[0]

    def scores_of(a, k, triangle=False):
        s = lax.dot_general(k, queries(a), (((1,), (1,)), ((), ())),
                            preferred_element_type=jnp.float32)
        blocks = [s[i * BLK:(i + 1) * BLK] for i in range(k.shape[0] // BLK)]
        if triangle:
            keys_at = lax.broadcasted_iota(jnp.int32, blocks[0].shape, 0)
            query_at = lax.broadcasted_iota(jnp.int32, blocks[0].shape, 1) % BLK
            blocks[0] = jnp.where(keys_at <= query_at, blocks[0], NEGATIVE)
        return blocks

    def weigh(blocks, negs, old):
        high = None
        for block, neg in zip(blocks, negs):
            part = fold(block, jnp.maximum)
            part = part if neg is None else part + neg
            high = part if high is None else jnp.maximum(high, part)
        peak = jnp.max(high, axis=0, keepdims=True) * SCALE
        if old is not None:
            peak = jnp.maximum(peak, old[0])
        amount, packed = None, []
        for block, neg in zip(blocks, negs):
            w = jnp.exp2(block * SCALE - (peak if neg is None else peak - neg))
            part = fold(w, jnp.add)
            amount = part if amount is None else amount + part
            packed.append(w.astype(jnp.bfloat16))
        shrink = None
        if old is not None:
            shrink = jnp.exp2(old[0] - peak)
            amount = amount + old[1] * shrink
        return peak, amount, shrink, jnp.concatenate(packed, axis=0)

    def attend(todo, old, triangle=False):
        scores = [scores_of(a, k, triangle) for a, k, _, _ in todo]
        soft = [weigh(blocks, negs, before(a) if old else None)
                for blocks, (a, _, _, negs) in zip(scores, todo)]
        done = []
        for (peak, amount, shrink, p), (a, _, vt, _) in zip(soft, todo):
            mix = jnp.dot(vt, p, preferred_element_type=jnp.float32)
            if old:
                mix = mix + acc[a] * shrink
            done.append((peak, amount, mix))
        return done

    def before(a):
        return top[a], total[a]

    def keep(todo, done):
        for (a, _, _, _), state in zip(todo, done):
            top[a], total[a], acc[a] = state

    def plane_block(a):
        rank, slab = slots[a], a // slab_blocks
        early = sel[slab * CAP + jnp.minimum(rank, CAP - 1)]
        late = rest[slab * others_count + jnp.maximum(rank - CAP, 0)]
        return jnp.where(rank < CAP, early, late)

    def near(slab):
        todo = []
        for i in range(slab_blocks):
            a = slab * slab_blocks + i
            both, negs = [plane_block(a)], [None]
            for j in range(slashes):
                at = a - slash_ref[j, c]
                both.append(plane_block(jnp.maximum(at, 0)))
                negs.append(jnp.where(at >= 0, 0.0, NEGATIVE))
            ks, vs = [x[:BLK] for x in both], [x[BLK:] for x in both]
            todo.append((a, jnp.concatenate(ks, axis=0), jnp.concatenate(vs, axis=0).T, negs))
        keep(todo, attend(todo, False, True))

    def on_far(a, g, count):
        negs = []
        for i in range(count * grain):
            gap = first + a - vert_ref[c, g * grain + i]
            negs.append(jnp.where((gap > 0) & jnp.logical_not(on_slash(gap)), 0.0, NEGATIVE))
        k = jnp.concatenate([pos[g * grain + i, :BLK] for i in range(count * grain)], axis=0)
        vt = jnp.concatenate([vtpos[g + i] for i in range(count)], axis=1)
        return a, k, vt, negs

    def far(slab, g, count):
        for part in range(0, slab_blocks, FAR):
            todo = [on_far(slab * slab_blocks + part + i, g, count) for i in range(FAR)]
            keep(todo, attend(todo, True))

    def back(_):
        k = jnp.concatenate([prev[i, :BLK] for i in range(slab_blocks)], axis=0)
        vt = jnp.concatenate([prev[i, BLK:] for i in range(slab_blocks)], axis=0).T
        todo = []
        for a in range(slab_blocks):
            negs = [jnp.where(on_slash(a + slab_blocks - prev_blocks[i]), 0.0, NEGATIVE)
                    for i in range(slab_blocks)]
            todo.append((a, k, vt, negs))
        keep(todo, attend(todo, True))

    def finish(slab, e, count):
        done = []
        for part in range(0, slab_blocks, FAR):
            done += attend([on_far(slab * slab_blocks + part + i, 0, count)
                            for i in range(FAR)], True)
        for i, (_, amount, mix) in enumerate(done):
            amount = jnp.sum(amount, axis=0, keepdims=True)
            out = (mix * (1.0 / amount)).astype(abuf.dtype).T
            for g in range(per_group):
                abuf[e, i * BLK:(i + 1) * BLK, g * HEAD_DIM:(g + 1) * HEAD_DIM] = (
                    out[g * BLK:(g + 1) * BLK])

    for e in others:
        slab = source(e)
        give_sel(e, c, slab).wait_recv()

    prompt = (o == outer - 2) & (core == 1)

    @pl.when(prompt)
    def _():
        prev_copy(0).start()

    def rest_here():
        for e in others:
            give_rest(e, c, source(e)).wait_recv()

    @pl.when(o < outer - 1)
    def _():
        def relay(i, _):
            chain(grains - 1 - i)

            @pl.when(prompt & (i == min(1, grains - 2)))
            def _():
                rest_here()
                prev_copy(1).start()

            return 0

        lax.fori_loop(0, grains - 1, relay, 0)

    @pl.when(o < outer - 2)
    def _():
        chain(0)

    @pl.when(jnp.logical_not(prompt))
    def _():
        rest_here()

    loads[2].wait()
    near(c)

    @pl.when(o == outer - 2)
    def _():
        chain(0)

    @pl.when((o < outer - 1) & jnp.logical_not(prompt))
    def _():
        start_prev()

    half = rows // 2
    mine = pl.ds(pl.multiple_of(core * half, half), half)
    theirs = pl.ds(pl.multiple_of(other * half, half), half)

    def return_copy(e, part, h, to):
        there = (theirs, mine)[part]
        return remote(abuf.at[e, there], attn.at[h, there], r_send.at[e, part],
                      r_recv.at[h, part], base + to)

    def turn_of(i):
        return inner - 1 - i

    first_slab = source(turn_of(0))

    def meet(e):
        give_q(e, c, source(e)).wait_recv()
        near(source(e))

    def links(low, high):
        lax.fori_loop(0, high - low, lambda i, z: (chain(high - 1 - i), z)[1], 0)

    ready = (o == outer - 1) & (core == 0)

    @pl.when(ready)
    def _():
        def ahead(i, _):
            meet(turn_of(i))
            if split:
                @pl.when(i == max(inner - 3, 0))
                def _():
                    links(split, grains)
                    far(c, split, group - split)
                    far(first_slab, split, group - split)

            return 0

        lax.fori_loop(0, inner - 1, ahead, 0)
        links(0, split if split else grains)

    def last(i, _):
        e = turn_of(i)
        slab = source(e)

        @pl.when((e > 0) & jnp.logical_not(ready))
        def _():
            meet(e)

        @pl.when((i == 0) & (o == outer - 1) & (core == 1))
        def _():
            links(0, grains)

        @pl.when((slab == 0) & (o > 0))
        def _():
            for part in range(2):
                prev_copy(part).wait_recv()
            back(0)

        lax.fori_loop(0, grains // group - 1,
                      lambda i, z: (far(slab, grains - (i + 1) * group, group), z)[1], 0)
        if split:
            begun = ready & ((i == 0) | (e == 0))

            @pl.when(begun)
            def _():
                finish(slab, e, split)

            @pl.when(jnp.logical_not(begun))
            def _():
                finish(slab, e, group)
        else:
            finish(slab, e, group)

        @pl.when(e > 0)
        def _():
            for part in range(2):
                return_copy(e, part, c, source(e)).start()

        return 0

    lax.fori_loop(0, inner, last, 0)

    weight_copy.wait()
    tiles = give.shape[0]
    def columns(t):
        return pl.ds(pl.multiple_of(t * tile, tile), tile)

    def swap(t):
        return pltpu.make_async_remote_copy(
            src_ref=give.at[t], dst_ref=take.at[t], send_sem=x_send.at[t], recv_sem=x_recv.at[t],
            device_id=(me, other), device_id_type=MESH,
        )

    def product(values, h, t):
        return jnp.dot(values, w_ref[span(h, width), columns(t)],
                       preferred_element_type=jnp.float32)

    def project_own(t, _):
        res[t] = product(abuf[0], c, t)
        return 0

    lax.fori_loop(0, tiles, project_own, 0, unroll=UNROLL)

    def returned(e, part):
        return_copy(e, part, peer(e), c).wait_recv()

    for e in others[:-1]:
        returned(e, 0)
        returned(e, 1)
        h = peer(e)

        def project_more(t, _, h=h):
            res[t] = res[t] + product(attn[h], h, t)
            return 0

        lax.fori_loop(0, tiles, project_more, 0, unroll=UNROLL)

    h_last = peer(others[-1])
    returned(others[-1], 0)

    def project_theirs(t, _):
        out = res[t, theirs, :] + product(attn[h_last, theirs, :], h_last, t)
        give[t] = out.astype(jnp.bfloat16)
        return 0

    for first_tile in range(0, tiles, UNROLL):
        lax.fori_loop(first_tile, first_tile + UNROLL, project_theirs, 0, unroll=UNROLL)
        for t in range(first_tile, first_tile + UNROLL):
            swap(t).start()

    returned(others[-1], 1)

    def project_mine(t, _):
        res[t, mine, :] = res[t, mine, :] + product(attn[h_last, mine, :], h_last, t)
        return 0

    lax.fori_loop(0, tiles, project_mine, 0, unroll=UNROLL)

    def add_up(t, _):
        swap(t).wait_recv()
        out_ref[:, columns(t)] = (res[t, mine, :] + take[t].astype(jnp.float32)).astype(out_ref.dtype)
        return 0

    lax.fori_loop(0, tiles, add_up, 0)

    def sent(t, _):
        swap(t).wait_send()
        return 0

    lax.fori_loop(0, tiles, sent, 0)
    for e in others:
        for hand in (give_sel, give_rest, give_q):
            hand(e, peer(e), c).wait_send()
        for part in range(2):
            return_copy(e, part, c, source(e)).wait_send()

    @pl.when(o < outer - 1)
    def _():
        for part in range(2):
            prev_copy(part).wait_send()

    def left(g, _):
        @pl.when(leaving(g))
        def _():
            chain_copy(g).wait_send()

        return 0

    lax.fori_loop(0, grains, left, 0)


def on_device(n, queries, keys, values, vertical, slash, out_weight):
    rows = queries.shape[0]
    inner = vertical.shape[0]
    per_group = queries.shape[1] // (inner * HEAD_DIM)
    width = per_group * HEAD_DIM
    slab_blocks = rows // BLK
    plane_blocks = inner * slab_blocks
    chosen = vertical.shape[1]
    model = out_weight.shape[1]
    grain = math.gcd(chosen, 4)
    grains = chosen // grain
    group = math.gcd(grains, 4)
    split = group // 2 if group == grains and inner > 1 else 0
    tile = math.gcd(model, 512)
    tiles = model // tile
    bf16, f32 = jnp.bfloat16, jnp.float32
    vmem = pl.BlockSpec(memory_space=pltpu.VMEM)
    smem = pl.BlockSpec(memory_space=pltpu.SMEM)
    hbm = pl.BlockSpec(memory_space=pl.ANY)
    dma = pltpu.SemaphoreType.DMA
    return pl.pallas_call(
        functools.partial(kernel, n, inner, per_group, tile, grain, group, split),
        out_shape=pltpu.VMEM((rows // 2, model), bf16),
        in_specs=[hbm] * 3 + [smem] * 2 + [hbm],
        out_specs=vmem,
        scratch_shapes=[
            pltpu.VMEM((slab_blocks, BLK, inner * HEAD_DIM), bf16),
            pltpu.VMEM((slab_blocks, BLK, inner * HEAD_DIM), bf16),
            pltpu.VMEM((inner, slab_blocks, 2 * BLK, HEAD_DIM), bf16),
            pltpu.VMEM((inner * CAP, 2 * BLK, HEAD_DIM), bf16),
            pltpu.VMEM((inner * (slab_blocks - CAP), 2 * BLK, HEAD_DIM), bf16),
            pltpu.SMEM((plane_blocks,), jnp.int32),
            pltpu.VMEM((plane_blocks, BLK, width), bf16),
            pltpu.VMEM((slab_blocks, 2 * BLK, HEAD_DIM), bf16),
            pltpu.VMEM((chosen, 2 * BLK, HEAD_DIM), bf16),
            pltpu.VMEM((chosen, 2 * BLK, HEAD_DIM), bf16),
            pltpu.VMEM((grains, HEAD_DIM, grain * BLK), bf16),
            pltpu.VMEM((plane_blocks, HEAD_DIM, per_group * BLK), f32),
            pltpu.VMEM((plane_blocks, 1, per_group * BLK), f32),
            pltpu.VMEM((plane_blocks, 8, per_group * BLK), f32),
            pltpu.VMEM((inner, rows, width), bf16),
            pltpu.VMEM((inner, rows, width), bf16),
            pltpu.VMEM(out_weight.shape, bf16),
            pltpu.VMEM((tiles, rows, tile), f32),
            pltpu.VMEM((tiles, rows // 2, tile), bf16),
            pltpu.VMEM((tiles, rows // 2, tile), bf16),
            dma((3,)),
            dma,
            dma((inner,)), dma((inner,)),
            dma((inner,)), dma((inner,)),
            dma((inner,)), dma((inner,)),
            dma((2,)), dma((2,)),
            dma((grains,)), dma((grains,)),
            dma((inner, 2)), dma((inner, 2)),
            dma((tiles,)), dma((tiles,)),
            pltpu.SemaphoreType.REGULAR,
        ],
        compiler_params=pltpu.CompilerParams(
            collective_id=0, has_side_effects=True, vmem_limit_bytes=60 * 2**20
        ),
    )(*(x.reshape(slab_blocks, BLK, -1) for x in (queries, keys, values)),
      vertical, slash.T, out_weight)


def solution(mesh):
    placed = (
        P("seq", "head"),
        P("seq", "head"),
        P("seq", "head"),
        P("head", None),
        P("head", None),
        P("head", None),
    )
    return jax.shard_map(
        functools.partial(on_device, mesh.shape["seq"]),
        mesh=mesh, in_specs=placed, out_specs=P(("seq", "head"), None), check_vma=False,
    )
```
